768 devices in a mesh: dp: 12 (over x, z_lo), expert: 64 (over y, z_hi, core).
Axes of the slice: x: 4, y: 8, z: 12 (z_hi: 4, z_lo: 3; z = z_hi * 3 + z_lo), core: 2. Of those that a mesh axis runs over, the one named last changes fastest.
Arguments:
- out_grad: bfloat16 [9216, 3072], P(('dp', 'expert')), may hold values from -6 to 6
- layer_input: bfloat16 [9216, 3072], P(('dp', 'expert')), may hold values from -6 to 6
- expert_ids: int32 [9216, 2], P(('dp', 'expert')), may hold values from 0 to 7, as said below
- gate_prob: float32 [9216, 2], P(('dp', 'expert')), may hold values from 0.05 to 1
- w_stack: bfloat16 [3, 3072, 8192], P(None, 'dp', 'expert'), may hold values from -0.109375 to 0.109375
- scale_exps: int32 [3, 24, 64], P(None, 'dp', 'expert'), may hold values from -1 to 1
Outputs:
- input_grad: bfloat16 [9216, 3072], P(('dp', 'expert'))
- weight_grads: float32 [3, 3072, 8192], P(None, 'dp', 'expert')
The draws below stay inside these ranges and needn't reach their ends.
Inputs may be any that keep to these rules, and one draw needn't show every extreme that they name: `expert_ids`: each row names two different experts. In each aligned block of 12 rows (the tokens of one device) between 1 and 3 rows name expert 0, and some blocks have exactly 3 in every draw.
All inputs are finite; a program needn't handle non-finite values.
Results may differ from the reference program's by a relative error of at most 0.015.
Values may be sent and summed in bfloat16 or wider, within the bound.
A program may use at most 32 MiB of HBM per device.

```python
import math
import jax
import jax.numpy as jnp
from jax import lax

D = 3072
FF = 8192
EXPERTS = 8
TOP = 2
TILE = 128
CAP = 3
TOK_DEV = 12
TOKENS = 9216
N_DP = 12
N_EXPERT = 64


def draw_expert_ids(key, part):
    block_count = TOKENS // TOK_DEV
    subkeys = jax.random.split(jax.random.fold_in(key, 11), 7)
    counts = jax.random.randint(subkeys[0], (block_count,), 1, CAP + 1)
    full_block = jax.random.randint(subkeys[1], (block_count,), 0, 4) == 0
    chosen = jax.random.randint(subkeys[2], (), 0, block_count)
    counts = jnp.where(full_block | (jnp.arange(block_count) == chosen), CAP, counts)
    ranks = jax.vmap(lambda subkey: jax.random.permutation(subkey, TOK_DEV))(jax.random.split(subkeys[3], block_count))
    routed = ranks < counts[:, None]
    first_pick = jax.random.randint(subkeys[4], (block_count, TOK_DEV), 1, EXPERTS)
    offset = jax.random.randint(subkeys[5], (block_count, TOK_DEV), 1, EXPERTS - 1)
    second = 1 + (first_pick - 1 + offset) % (EXPERTS - 1)
    flipped = jax.random.randint(subkeys[6], (block_count, TOK_DEV), 0, 2) == 1
    column_left = jnp.where(routed, jnp.where(flipped, first_pick, 0), first_pick)
    column_right = jnp.where(routed, jnp.where(flipped, 0, first_pick), second)
    return jnp.stack([column_left, column_right], axis=-1).reshape(TOKENS, 2).astype(jnp.int32)


def with_ends(entries, stream_key, low, high):
    longest = entries.shape.index(max(entries.shape))
    spots = []
    for shift in (0, 1):
        where = [jax.random.randint(jax.random.fold_in(stream_key, axis), (), 0, length) for axis, length in enumerate(entries.shape)]
        where[longest] = (where[longest] + shift) % entries.shape[longest]
        spots.append(tuple(where))
    return entries.at[spots[0]].set(low).at[spots[1]].set(high)


def levels(rng, shape, cuts, low, high):
    def one(axis_at, parts):
        steps = jax.random.uniform(jax.random.fold_in(jax.random.fold_in(rng, 6), axis_at), (parts,), jnp.float32, low / len(cuts), high / len(cuts))
        return jnp.repeat(jnp.exp(steps), shape[axis_at] // parts).reshape((-1,) + (1,) * (len(shape) - axis_at - 1))

    loudness = one(*cuts[0])
    for cut in cuts[1:]:
        loudness = loudness * one(*cut)
    return loudness


def scatter_about(stream_key, dims, deviation, limit, pieces=(), kind=jnp.bfloat16):
    drawn = jax.random.normal(stream_key, dims, jnp.float32) * deviation
    if len(pieces) > 0:
        drawn = levels(stream_key, dims, pieces, -0.22, 0.18) * drawn
    return jnp.clip(drawn, min=-limit, max=limit).astype(kind)


def setup_inputs(seed: int = 0) -> dict:
    key_list = jax.random.split(jax.random.key(seed), 7)
    return {
        "out_grad": scatter_about(key_list[0], (TOKENS, D), 1.0, 6.0, ((0, 768),)),
        "layer_input": scatter_about(key_list[1], (TOKENS, D), 1.0, 6.0, ((0, 768),)),
        "expert_ids": draw_expert_ids(jax.random.fold_in(key_list[6], 71), 0),
        "gate_prob": jnp.clip(jnp.exp(math.log(1.0) - 2.9957323 * jax.random.uniform(key_list[3], (TOKENS, TOP), jnp.float32) ** levels(key_list[3], (TOKENS, TOP), ((0, 768),), -0.2, 0.2)), 0.05, 1.0),
        "w_stack": scatter_about(key_list[4], (3, D, FF), D ** -0.5, 0.109375, ((1, 12), (2, 64))),
        "scale_exps": with_ends(jax.random.randint(key_list[5], (3, D // TILE, FF // TILE), -1, 2), jax.random.fold_in(key_list[5], 1), -1, 1).astype(jnp.int32),
    }


def dequantize(w_stack, scale_exps):
    factor = jnp.exp2(scale_exps.astype(jnp.float32))
    scaled = w_stack.astype(jnp.float32).reshape(3, D // TILE, TILE, FF // TILE, TILE) * factor[:, :, None, :, None]
    return scaled.reshape(3, D, FF).astype(jnp.bfloat16)


def contract_rows(left, right):
    return lax.dot_general(left, right, (((0,), (0,)), ((), ())), preferred_element_type=jnp.float32)


def back_project(grad_rows, matrix):
    return lax.dot_general(grad_rows, matrix, (((1,), (1,)), ((), ())), preferred_element_type=jnp.float32)


def expert_backward(routed_input, routed_grad, weights):
    gate_value = jnp.dot(routed_input, weights[0], preferred_element_type=jnp.float32)
    up_value = jnp.dot(routed_input, weights[1], preferred_element_type=jnp.float32)
    down_back = jnp.dot(routed_grad, weights[2], preferred_element_type=jnp.float32)
    gate_sigmoid = jax.nn.sigmoid(gate_value)
    gate_act = gate_value * gate_sigmoid
    gate_grad = (down_back * up_value * gate_sigmoid * (1.0 + gate_value * (1.0 - gate_sigmoid))).astype(jnp.bfloat16)
    up_grad = (down_back * gate_act).astype(jnp.bfloat16)
    hidden = (gate_act * up_value).astype(jnp.bfloat16)
    returned = back_project(gate_grad, weights[0]) + back_project(up_grad, weights[1])
    partial_value = jnp.stack([contract_rows(routed_input, gate_grad), contract_rows(routed_input, up_grad), contract_rows(routed_grad, hidden)])
    return returned, partial_value


def reference(out_grad, layer_input, expert_ids, gate_prob, w_stack, scale_exps):
    weights = dequantize(w_stack, scale_exps)
    routed = expert_ids == 0
    routed_mask = jnp.any(routed, axis=1)
    expert_prob = jnp.sum(jnp.where(routed, gate_prob, 0.0), axis=1)
    block_count = out_grad.shape[0] // TOK_DEV
    block_mask = routed_mask.reshape(block_count, TOK_DEV)
    slot_index = jnp.cumsum(block_mask.astype(jnp.int32), axis=1) - 1
    places = jnp.arange(CAP, dtype=jnp.int32)
    slot_hit = (slot_index[:, None, :] == places[None, :, None]) & block_mask[:, None, :]
    positions = jnp.arange(TOK_DEV, dtype=jnp.int32)
    source = jnp.sum(jnp.where(slot_hit, positions[None, None, :], 0), axis=2)
    source = (source + (jnp.arange(block_count, dtype=jnp.int32) * TOK_DEV)[:, None]).reshape(-1)
    slot_valid = jnp.any(slot_hit, axis=2).reshape(-1)
    slot_input = jnp.where(slot_valid[:, None], layer_input[source], jnp.zeros((), jnp.bfloat16))
    slot_grad = jnp.where(slot_valid[:, None], expert_prob[source][:, None] * out_grad[source].astype(jnp.float32), 0.0).astype(jnp.bfloat16)
    slot_rows = N_EXPERT * CAP
    group_input = slot_input.reshape(N_DP, slot_rows, D)
    group_grad = slot_grad.reshape(N_DP, slot_rows, D)

    def group_step(total, pair):
        returned, partial_value = expert_backward(pair[0], pair[1], weights)
        rounded = lax.optimization_barrier(partial_value.astype(jnp.bfloat16))
        return total + rounded.astype(jnp.float32), returned

    weight_grads, returned = lax.scan(group_step, jnp.zeros((3, D, FF), jnp.float32), (group_input, group_grad))
    returned = returned.reshape(block_count, CAP, D)
    picked = jnp.take_along_axis(returned, jnp.clip(slot_index, 0, CAP - 1)[:, :, None], axis=1)
    input_grad = jnp.where(block_mask[:, :, None], picked, 0.0).reshape(-1, D).astype(jnp.bfloat16)
    return input_grad, weight_grads
```

```python
import functools

import jax
import jax.numpy as jnp
from jax import lax
from jax.experimental import pallas as pl
from jax.experimental.pallas import tpu as pltpu
from jax.sharding import Mesh
from jax.sharding import PartitionSpec as P

TILE = 128
CAP = 3
PAD = 8
MESH = pl.DeviceIdType.MESH
AXES = ("x", "zl", "y", "zh", "core")
SIZES = (4, 3, 8, 4, 2)
F32 = jnp.float32
BF16 = jnp.bfloat16


def dot(left, right, contract=((1,), (0,))):
    return lax.dot_general(left, right, (contract, ((), ())), preferred_element_type=F32)


class Net:
    def __init__(self, send_sems, recv_sems):
        self.send_sems, self.recv_sems, self.copies = send_sems, recv_sems, []

    def send(self, src, dst, **where):
        i = len(self.copies)
        copy = pltpu.make_async_remote_copy(
            src_ref=src,
            dst_ref=dst,
            send_sem=self.send_sems.at[i],
            recv_sem=self.recv_sems.at[i],
            device_id=where,
            device_id_type=MESH,
        )
        copy.start()
        self.copies.append(copy)
        return copy


def kernel(
    sizes, og_ref, li_ref, ids_ref, prob_ref, w_ref, exp_ref, ig_ref, wg_ref,
    W, A, AR, HIT, Z, S, GU, HID, CX, CR, OWN, YS, YR, ZS, ZR, FR,
    G2, R2, G1, R1, GO, GS, GR, send_sems, recv_sems,
):
    nx, nz, ny, nh, _ = sizes
    x, zl, y, zh, core = (lax.axis_index(a) for a in AXES)
    d = li_ref.shape[1]
    half = d // 2
    rows, block = 6 * nh, w_ref.shape[1]
    net = Net(send_sems, recv_sems)

    def turn(at, by, n):
        return lax.rem(at + by + n, n)

    xs = {s: turn(x, s, nx) for s in (1, -1)}
    ys = {s: turn(y, s, ny) for s in (1, -1)}
    hs = {s: turn(zh, s, nh) for s in (1, -1)}
    other = 1 - core

    def piece(xx, zz):
        return pl.ds(pl.multiple_of((xx * nz + zz) * block, block), block)

    def halfpiece(xx, zz, part):
        size = block // 2
        return pl.ds(pl.multiple_of((xx * nz + zz) * block + part * size, size), size)

    for k in range(3):
        for t in range(block // TILE):
            e = exp_ref[t, :, k : k + 1]
            factor = jnp.where(e > 0, 2.0, jnp.where(e < 0, 0.5, 1.0)).astype(F32)
            scaled = (w_ref[k, t * TILE : (t + 1) * TILE, :].astype(F32) * factor).astype(BF16)
            at = pl.multiple_of((x * nz + zl) * block + t * TILE, TILE)
            W[pl.ds(at, TILE), k * TILE : (k + 1) * TILE] = scaled

    tokens = ids_ref.shape[1]
    r0, r1 = ids_ref[0:1, :] == 0, ids_ref[1:2, :] == 0
    routed = jnp.broadcast_to(jnp.where(r0 | r1, 1.0, 0.0).astype(F32), (PAD, tokens))
    prob = jnp.where(r0, prob_ref[0:1, :], 0.0) + jnp.where(r1, prob_ref[1:2, :], 0.0)
    upto = (
        lax.broadcasted_iota(jnp.int32, (tokens, tokens), 0)
        <= lax.broadcasted_iota(jnp.int32, (tokens, tokens), 1)
    )
    place = dot(routed.astype(BF16), jnp.where(upto, 1.0, 0.0).astype(BF16))
    wanted = (lax.broadcasted_iota(jnp.int32, (PAD, tokens), 0) - 3 * core + 1).astype(F32)
    hit = jnp.where(place == wanted, routed, 0.0)
    HIT[...] = hit
    hit_b = hit.astype(BF16)
    A[0] = dot(hit_b, li_ref[...]).astype(BF16)
    slot_prob = jnp.sum(hit * prob, axis=1, keepdims=True)
    A[1] = (slot_prob * dot(hit_b, og_ref[...])).astype(BF16)

    barrier = pltpu.get_barrier_semaphore()
    greeted = [dict(core=other)]
    if nx > 1:
        greeted += [dict(x=xs[1]), dict(x=xs[-1])]
    greeted += [dict(zl=turn(zl, s, nz)) for s in range(1, nz)]
    if ny > 1:
        greeted += [dict(y=ys[1]), dict(y=ys[-1])]
    if nh > 1:
        greeted += [dict(zh=hs[1]), dict(zh=hs[-1])]
    for where in greeted:
        pl.semaphore_signal(barrier, inc=1, device_id=where, device_id_type=MESH)
    pl.semaphore_wait(barrier, len(greeted))

    a_in = net.send(A.at[other], AR, core=other)
    own = W.at[piece(x, zl)]

    def spread(ref):
        return {s: net.send(ref, ref, x=xs[s]) for s in (1, -1)} if nx > 1 else None

    def relay(zz):
        if nx == 1:
            return None
        out = {}
        for s, part in ((1, 0), (-1, 1)):
            ref = W.at[halfpiece(xs[-s], zz, part)]
            out[s] = net.send(ref, ref, x=xs[s])
        return out

    def arrive(copies):
        for s in (1, -1):
            if copies is not None:
                copies[s].wait_recv()

    w_own = spread(own)
    w_z = [net.send(own, own, zl=turn(zl, s, nz)) for s in range(1, nz)]
    relays = []

    a_in.wait_recv()
    Z[zh] = A[core] + AR[...]
    z_in = {s: net.send(Z.at[zh], Z.at[zh], zh=hs[s]) for s in (1, -1)} if nh > 1 else None

    w_x = [(zl, w_own)]
    if nz > 1:
        w_z[0].wait_recv()
        zz = turn(zl, -1, nz)
        w_x.append((zz, spread(W.at[piece(x, zz)])))

    if nh > 1:
        arrive(z_in)
        z_far = []
        for s, part in ((1, 0), (-1, 1)):
            ref = Z.at[hs[-s], :, part * (half) : (part + 1) * half]
            z_far.append(net.send(ref, ref, zh=hs[s]))

    arrive(w_x[0][1])
    relays.append(relay(w_x[0][0]))
    if nz > 2:
        w_z[1].wait_recv()
        zz = turn(zl, -2, nz)
        w_x.append((zz, spread(W.at[piece(x, zz)])))

    if nh > 1:
        for copy in z_far:
            copy.wait_recv()

    packed = lax.broadcasted_iota(jnp.int32, (rows, nh * PAD), 0)
    padded = lax.broadcasted_iota(jnp.int32, (rows, nh * PAD), 1)
    same = padded == (packed // 6) * PAD + lax.rem(packed, 6)
    pack = jnp.where(same, 1.0, 0.0).astype(BF16)

    def yrows(yy):
        return pl.ds(pl.multiple_of(yy * rows, 8), rows)

    def ypart(yy, k):
        return S.at[core, yrows(yy), k * half : (k + 1) * half]

    S[core, yrows(y), :] = dot(pack, Z[...].reshape(nh * PAD, d)).astype(BF16)

    partner = []

    def to_partner(ref):
        partner.append(net.send(ref, ref, core=other))

    hops = ny // 2
    if ny > 1:
        y_in = {(s, k): net.send(ypart(y, k), ypart(y, k), y=ys[s]) for k in (0, 1) for s in (1, -1)}
    to_partner(S.at[core, yrows(y)])

    if nz > 1:
        arrive(w_x[1][1])
        relays.append(relay(w_x[1][0]))

    for hop in range(1, hops + 1):
        later = {}
        for k in (0, 1):
            for s in (1, -1):
                if (s, k) not in y_in:
                    continue
                y_in[s, k].wait_recv()
                ref = ypart(turn(y, -s * hop, ny), k)
                if hop < hops - 1 or (hop == hops - 1 and k == (0 if s == 1 else 1)):
                    later[s, k] = net.send(ref, ref, y=ys[s])
                to_partner(ref)
        y_in = later
        if hop == 1 and nz > 2:
            arrive(w_x[2][1])
            relays.append(relay(w_x[2][0]))

    for copies in relays:
        arrive(copies)
    for copy in partner:
        copy.wait_recv()

    total = rows * ny
    gate_up = dot(S[0, 0:total, :], W[:, 0 : 2 * TILE])
    back = dot(S[1, 0:total, :], W[:, 2 * TILE : 3 * TILE])
    gate, up = gate_up[:, 0:TILE], gate_up[:, TILE : 2 * TILE]
    sig = jax.nn.sigmoid(gate)
    act = gate * sig
    GU[:, 0:TILE] = (back * up * sig * (1.0 + gate * (1.0 - sig))).astype(BF16)
    GU[:, TILE : 2 * TILE] = (back * act).astype(BF16)
    HID[...] = (act * up).astype(BF16)

    step = block if half % block == 0 else TILE

    def back_part(which, put):
        for j in range(half // step):
            at = pl.multiple_of(which * half + j * step, step)
            put(j * step, dot(GU[...], W[pl.ds(at, step), 0 : 2 * TILE], ((1,), (1,))))

    def put_sent(at, value):
        CX[:, at : at + step] = value.astype(BF16)

    def put_own(at, value):
        OWN[:, at : at + step] = value

    def grads(xx, zz):
        at = piece(xx, zz)
        return (
            dot(GU[...], S[0, 0:total, at], ((0,), (0,))),
            dot(HID[...], S[1, 0:total, at], ((0,), (0,))),
        )

    gu_rows, all_rows = 2 * TILE, 3 * TILE
    mid = all_rows // 2

    back_part(other, put_sent)
    c_in = net.send(CX, CR, core=other)

    order = [turn(zl, s, nz) for s in range(1, nz)] + [zl]
    g2_in = []
    if nx > 1:
        for i, zz in enumerate(order):
            first, second = grads(turn(x, 2, nx), zz)
            G2[i, 0:gu_rows, :] = first.astype(BF16)
            G2[i, gu_rows:all_rows, :] = second.astype(BF16)
            g2_in.append(
                {
                    s: net.send(G2.at[i, part * mid : (part + 1) * mid], R2.at[part, i], x=xs[s])
                    for s, part in ((1, 0), (-1, 1))
                }
            )

    back_part(core, put_own)
    c_in.wait_recv()
    OWN[...] += CR[...].astype(F32)

    g1_in = []

    def send_near(i):
        if nx == 1:
            return
        arrive(g2_in[i])
        copies = {}
        for s, part in ((1, 0), (-1, 1)):
            first, second = grads(xs[s], order[i])
            G = jnp.concatenate([first, second], axis=0)
            lo, hi = part * mid, (part + 1) * mid
            G1[part, i, lo:hi, :] = (G[lo:hi] + R2[part, i].astype(F32)).astype(BF16)
            lo, hi = (1 - part) * mid, (2 - part) * mid
            G1[part, i, lo:hi, :] = G[lo:hi].astype(BF16)
            copies[s] = net.send(G1.at[part, i], R1.at[part, i], x=xs[s])
        g1_in.append(copies)

    def summed_here(i):
        first, second = grads(x, order[i])
        GO[0:gu_rows, :] = first
        GO[gu_rows:all_rows, :] = second
        if nx > 1:
            arrive(g1_in[i])
            GO[...] += R1[0, i].astype(F32) + R1[1, i].astype(F32)

    quarter = half // 2
    y_in = {}

    def y_step(hop):
        far = hops + 1 - hop
        copies = {}
        for s, part in ((1, 0), (-1, 1)):
            dest = yrows(turn(y, s * far, ny))
            mine = slice(part * quarter, (part + 1) * quarter)
            if hop == 1:
                YS[part, 0, :, mine] = OWN[dest, mine].astype(BF16)
                copies[s] = net.send(YS.at[part, 0, :, mine], YR.at[part, 0, :, mine], y=ys[s])
                continue
            y_in[s].wait_recv()
            if hop == 2:
                theirs = slice((1 - part) * quarter, (2 - part) * quarter)
                value = OWN[dest, mine] + YR[part, 0, :, mine].astype(F32)
                YS[part, 1, :, mine] = value.astype(BF16)
                YS[part, 1, :, theirs] = OWN[dest, theirs].astype(BF16)
            else:
                value = OWN[dest, :] + YR[part, hop - 2].astype(F32)
                YS[part, hop - 1] = value.astype(BF16)
            copies[s] = net.send(YS.at[part, hop - 1], YR.at[part, hop - 1], y=ys[s])
        y_in.update(copies)

    if ny > 1:
        y_step(1)
    for i in range(nz):
        send_near(i)
        if ny > 1 and i + 2 <= hops:
            y_step(i + 2)
    for hop in range(nz + 2, hops + 1):
        y_step(hop)

    gz_in = []

    def to_zl(i):
        summed_here(i)
        GS[i] = GO[...].astype(BF16)
        gz_in.append(net.send(GS.at[i], GR.at[i], zl=order[i]))

    if nz > 1:
        to_zl(0)

    mine_y = OWN[yrows(y), :]
    if ny > 1:
        for s, part in ((1, 0), (-1, 1)):
            y_in[s].wait_recv()
            mine_y = mine_y + YR[part, hops - 1].astype(F32)
    spread_rows = dot(pack, mine_y.astype(BF16), ((0,), (0,)))
    ZS[...] = spread_rows.reshape(nh, PAD, half).astype(BF16)

    def zpart(part):
        return slice(part * quarter, (part + 1) * quarter)

    if nh > 1:
        far = turn(zh, 2, nh)
        z_in = {
            s: net.send(ZS.at[far, :, zpart(part)], ZR.at[part, 0, :, zpart(part)], zh=hs[s])
            for s, part in ((1, 0), (-1, 1))
        }
    if nz > 2:
        to_zl(1)
    if nh > 1:
        nearer = {}
        for s, part in ((1, 0), (-1, 1)):
            z_in[s].wait_recv()
            mine, theirs = zpart(part), zpart(1 - part)
            value = ZS[hs[s], :, mine].astype(F32) + ZR[part, 0, :, mine].astype(F32)
            ZR[part, 1, :, mine] = value.astype(BF16)
            ZR[part, 1, :, theirs] = ZS[hs[s], :, theirs]
            nearer[s] = net.send(ZR.at[part, 1], ZR.at[part, 2], zh=hs[s])

    summed_here(nz - 1)

    final = ZS[zh].astype(F32)
    if nh > 1:
        for s, part in ((1, 0), (-1, 1)):
            nearer[s].wait_recv()
            final = final + ZR[part, 2].astype(F32)
    FR[core] = final.astype(BF16)
    f_in = net.send(FR.at[core], FR.at[core], core=other)

    for i, copy in enumerate(gz_in):
        copy.wait_recv()
        GO[...] += GR[i].astype(F32)
    for k in range(3):
        wg_ref[k] = GO[k * TILE : (k + 1) * TILE, :].T

    f_in.wait_recv()
    hit_b = HIT[...].astype(BF16)
    for c in (0, 1):
        ig_ref[:, c * half : (c + 1) * half] = dot(hit_b, FR[c], ((0,), (0,))).astype(BF16)

    for copy in net.copies:
        copy.wait_send()


def per_device(sizes, out_grad, layer_input, expert_ids, gate_prob, w_stack, scale_exps):
    nx, nz, ny, nh, _ = sizes
    tokens, d = layer_input.shape
    block = w_stack.shape[1]
    half, rows, wide = d // 2, 6 * nh, 3 * TILE
    total = rows * ny
    hops = max(ny // 2, 1)
    held = total + 8 if total % 16 == 0 else total
    vmem = pl.BlockSpec(memory_space=pltpu.VMEM)
    scratch = [
        pltpu.VMEM((d, wide), BF16),
        pltpu.VMEM((2, PAD, d), BF16),
        pltpu.VMEM((PAD, d), BF16),
        pltpu.VMEM((PAD, tokens), F32),
        pltpu.VMEM((nh, PAD, d), BF16),
        pltpu.VMEM((2, held, d), BF16),
        pltpu.VMEM((total, 2 * TILE), BF16),
        pltpu.VMEM((total, TILE), BF16),
        pltpu.VMEM((total, half), BF16),
        pltpu.VMEM((total, half), BF16),
        pltpu.VMEM((total, half), F32),
        pltpu.VMEM((2, hops, rows, half), BF16),
        pltpu.VMEM((2, hops, rows, half), BF16),
        pltpu.VMEM((nh, PAD, half), BF16),
        pltpu.VMEM((2, 3, PAD, half), BF16),
        pltpu.VMEM((2, PAD, half), BF16),
        pltpu.VMEM((nz, wide, block), BF16),
        pltpu.VMEM((2, nz, wide // 2, block), BF16),
        pltpu.VMEM((2, nz, wide, block), BF16),
        pltpu.VMEM((2, nz, wide, block), BF16),
        pltpu.VMEM((wide, block), F32),
        pltpu.VMEM((nz, wide, block), BF16),
        pltpu.VMEM((nz, wide, block), BF16),
        pltpu.SemaphoreType.DMA((96,)),
        pltpu.SemaphoreType.DMA((96,)),
    ]
    return pl.pallas_call(
        functools.partial(kernel, sizes),
        out_shape=(
            jax.ShapeDtypeStruct((tokens, d), BF16),
            jax.ShapeDtypeStruct(w_stack.shape, F32),
        ),
        in_specs=[vmem] * 6,
        out_specs=(vmem, vmem),
        scratch_shapes=scratch,
        compiler_params=pltpu.CompilerParams(
            collective_id=0, has_side_effects=True, vmem_limit_bytes=48 * 1024 * 1024
        ),
        name="expert_backward",
    )(
        out_grad,
        layer_input,
        expert_ids.T,
        gate_prob.T,
        w_stack,
        jnp.transpose(scale_exps, (1, 2, 0)),
    )


def build(devices, sizes):
    split = Mesh(devices.reshape(sizes), AXES)
    tokens = P(AXES, None)
    weights = P(None, ("x", "zl"), ("y", "zh", "core"))
    return jax.shard_map(
        functools.partial(per_device, sizes),
        mesh=split,
        in_specs=(tokens, tokens, tokens, tokens, weights, weights),
        out_specs=(tokens, weights),
        check_vma=False,
    )


def solution(mesh):
    return build(mesh.devices, SIZES)
```

```python
import functools

import jax
import jax.numpy as jnp
from jax import lax
from jax.experimental import pallas as pl
from jax.experimental.pallas import tpu as pltpu
from jax.sharding import Mesh
from jax.sharding import PartitionSpec as P

TILE = 128
CAP = 3
PAD = 8
MESH = pl.DeviceIdType.MESH
AXES = ("x", "zl", "y", "zh", "core")
SIZES = (4, 3, 8, 4, 2)
F32 = jnp.float32
BF16 = jnp.bfloat16


def dot(left, right, contract=((1,), (0,))):
    return lax.dot_general(left, right, (contract, ((), ())), preferred_element_type=F32)


class Net:
    def __init__(self, send_sems, recv_sems):
        self.send_sems, self.recv_sems, self.copies = send_sems, recv_sems, []

    def send(self, src, dst, **where):
        i = len(self.copies)
        copy = pltpu.make_async_remote_copy(
            src_ref=src,
            dst_ref=dst,
            send_sem=self.send_sems.at[i],
            recv_sem=self.recv_sems.at[i],
            device_id=where,
            device_id_type=MESH,
        )
        copy.start()
        self.copies.append(copy)
        return copy


def kernel(
    sizes, og_hbm, li_hbm, ids_hbm, prob_hbm, w_hbm, exp_hbm, ig_ref, wg_ref,
    og_ref, li_ref, ids_ref, prob_ref, w_ref, exp_ref,
    W, A, AR, HIT, Z, S, GU, GT, HT, CX, CR, OWN, YS, YR, ZS, ZR, FR,
    G2, R2, G1, R1, GO, GS, GR, send_sems, recv_sems, load_sems, known,
):
    nx, nz, ny, nh, _ = sizes
    x, zl, y, zh, core = (lax.axis_index(a) for a in AXES)
    d = li_ref.shape[1]
    half = d // 2
    rows, block = 6 * nh, w_ref.shape[1]
    hops = ny // 2
    net = Net(send_sems, recv_sems)

    def turn(at, by, n):
        return lax.rem(at + by + n, n)

    xs = {s: turn(x, s, nx) for s in (1, -1)}
    ys = {s: turn(y, s, ny) for s in (1, -1)}
    hs = {s: turn(zh, s, nh) for s in (1, -1)}
    other = 1 - core

    barrier = pltpu.get_barrier_semaphore()
    greeted = [dict(core=other)]
    if nx > 1:
        greeted += [dict(x=xs[1]), dict(x=xs[-1])]
    greeted += [dict(zl=turn(zl, s, nz)) for s in range(1, nz)]
    if ny > 1:
        greeted += [dict(y=ys[1]), dict(y=ys[-1])]
    if nh > 1:
        greeted += [dict(zh=hs[1]), dict(zh=hs[-1])]
    for where in greeted:
        pl.semaphore_signal(barrier, inc=1, device_id=where, device_id_type=MESH)

    pairs = [
        (w_hbm, w_ref), (exp_hbm, exp_ref), (ids_hbm, ids_ref), (prob_hbm, prob_ref),
        (li_hbm, li_ref), (og_hbm, og_ref),
    ]
    loads = [pltpu.make_async_copy(src, dst, load_sems.at[i]) for i, (src, dst) in enumerate(pairs)]
    for load in loads:
        load.start()

    def piece(xx, zz):
        return pl.ds(pl.multiple_of((xx * nz + zz) * block, block), block)

    def halfpiece(xx, zz, part):
        size = block // 2
        return pl.ds(pl.multiple_of((xx * nz + zz) * block + part * size, size), size)

    def got(copy, name):
        with jax.named_scope(name):
            copy.wait_recv()

    def arrive(copies, name):
        for s in (1, -1):
            if copies is not None:
                got(copies[s], name)

    for load in loads[2:]:
        load.wait()
    tokens = ids_ref.shape[1]
    r0, r1 = ids_ref[0:1, :] == 0, ids_ref[1:2, :] == 0
    routed = jnp.broadcast_to(jnp.where(r0 | r1, 1.0, 0.0).astype(F32), (PAD, tokens))
    prob = jnp.where(r0, prob_ref[0:1, :], 0.0) + jnp.where(r1, prob_ref[1:2, :], 0.0)
    upto = (
        lax.broadcasted_iota(jnp.int32, (tokens, tokens), 0)
        <= lax.broadcasted_iota(jnp.int32, (tokens, tokens), 1)
    )
    place = dot(routed.astype(BF16), jnp.where(upto, 1.0, 0.0).astype(BF16))
    wanted = (lax.broadcasted_iota(jnp.int32, (PAD, tokens), 0) - 3 * core + 1).astype(F32)
    hit = jnp.where(place == wanted, routed, 0.0)
    HIT[...] = hit
    hit_b = hit.astype(BF16)
    A[0] = dot(hit_b, li_ref[...]).astype(BF16)
    slot_prob = jnp.sum(hit * prob, axis=1, keepdims=True)
    A[1] = (slot_prob * dot(hit_b, og_ref[...])).astype(BF16)

    for load in loads[:2]:
        load.wait()
    for k in range(3):
        for t in range(block // TILE):
            e = exp_ref[t, :, k : k + 1]
            factor = jnp.where(e > 0, 2.0, jnp.where(e < 0, 0.5, 1.0)).astype(F32)
            scaled = (w_ref[k, t * TILE : (t + 1) * TILE, :].astype(F32) * factor).astype(BF16)
            at = pl.multiple_of((x * nz + zl) * block + t * TILE, TILE)
            W[pl.ds(at, TILE), k * TILE : (k + 1) * TILE] = scaled

    with jax.named_scope("greet"):
        pl.semaphore_wait(barrier, len(greeted))
    if nh > 1:
        for s in (1, -1):
            pl.semaphore_signal(known, inc=1, device_id=dict(zh=hs[s]), device_id_type=MESH)

    a_in = net.send(A.at[other], AR, core=other)
    own = W.at[piece(x, zl)]

    def spread(ref):
        return {s: net.send(ref, ref, x=xs[s]) for s in (1, -1)} if nx > 1 else None

    def relay(zz):
        if nx == 1:
            return None
        out = {}
        for s, part in ((1, 0), (-1, 1)):
            ref = W.at[halfpiece(xs[-s], zz, part)]
            out[s] = net.send(ref, ref, x=xs[s])
        return out

    w_x = [(zl, spread(own))]
    relays = []

    got(a_in, "a")
    Z[zh] = A[core] + AR[...]
    if nh > 1:
        z_in = {s: net.send(Z.at[zh], Z.at[zh], zh=hs[s]) for s in (1, -1)}
    w_z = []
    if nz > 1:
        w_z.append(net.send(own, own, zl=turn(zl, 1, nz)))
    if nh > 1:
        arrive(z_in, "zh")
        z_far = []
        for s, part in ((1, 0), (-1, 1)):
            ref = Z.at[hs[-s], :, part * half : (part + 1) * half]
            z_far.append(net.send(ref, ref, zh=hs[s]))
    if nz > 2:
        w_z.append(net.send(own, own, zl=turn(zl, 2, nz)))

    arrive(w_x[0][1], "wx0")
    relays.append(relay(w_x[0][0]))
    if nz > 1:
        got(w_z[0], "wz0")
        zz = turn(zl, -1, nz)
        w_x.append((zz, spread(W.at[piece(x, zz)])))

    if nh > 1:
        for copy in z_far:
            got(copy, "zfar")

    packed = lax.broadcasted_iota(jnp.int32, (rows, nh * PAD), 0)
    padded = lax.broadcasted_iota(jnp.int32, (rows, nh * PAD), 1)
    same = padded == (packed // 6) * PAD + lax.rem(packed, 6)
    pack = jnp.where(same, 1.0, 0.0).astype(BF16)

    def yrows(yy):
        return pl.ds(pl.multiple_of(yy * rows, 8), rows)

    def ypart(yy, k):
        return S.at[core, yrows(yy), k * half : (k + 1) * half]

    S[core, yrows(y), :] = dot(pack, Z[...].reshape(nh * PAD, d)).astype(BF16)

    partner = []

    def to_partner(ref):
        partner.append(net.send(ref, ref, core=other))

    if ny > 1:
        y_in = {(s, k): net.send(ypart(y, k), ypart(y, k), y=ys[s]) for k in (0, 1) for s in (1, -1)}
    to_partner(S.at[core, yrows(y)])

    if nz > 2:
        got(w_z[1], "wz1")
        zz = turn(zl, -2, nz)
        w_x.append((zz, spread(W.at[piece(x, zz)])))

    def relay_next():
        at = len(relays)
        if at < nz:
            arrive(w_x[at][1], f"wx{at}")
            relays.append(relay(w_x[at][0]))

    for hop in range(1, hops + 1):
        later = {}
        for k in (0, 1):
            for s in (1, -1):
                if (s, k) not in y_in:
                    continue
                got(y_in[s, k], f"y{hop}")
                ref = ypart(turn(y, -s * hop, ny), k)
                if hop < hops - 1 or (hop == hops - 1 and k == (0 if s == 1 else 1)):
                    later[s, k] = net.send(ref, ref, y=ys[s])
                to_partner(ref)
        y_in = later
        relay_next()
    for _ in range(nz):
        relay_next()

    for copies in relays:
        arrive(copies, "wfar")
    for copy in partner:
        got(copy, "partner")

    total = rows * ny
    gate_up = dot(S[0, 0:total, :], W[:, 0 : 2 * TILE])
    back = dot(S[1, 0:total, :], W[:, 2 * TILE : 3 * TILE])
    gate, up = gate_up[:, 0:TILE], gate_up[:, TILE : 2 * TILE]
    sig = jax.nn.sigmoid(gate)
    act = gate * sig
    gate_grad = back * up * sig * (1.0 + gate * (1.0 - sig))
    up_grad = back * act
    GU[:, 0:TILE] = gate_grad.astype(BF16)
    GU[:, TILE : 2 * TILE] = up_grad.astype(BF16)
    GT[0:TILE, :] = gate_grad.T.astype(BF16)
    GT[TILE : 2 * TILE, :] = up_grad.T.astype(BF16)
    HT[...] = (act * up).T.astype(BF16)

    step = block if half % block == 0 else TILE

    def back_part(which, put):
        for j in range(half // step):
            at = pl.multiple_of(which * half + j * step, step)
            put(j * step, dot(GU[...], W[pl.ds(at, step), 0 : 2 * TILE], ((1,), (1,))))

    def put_sent(at, value):
        CX[:, at : at + step] = value.astype(BF16)

    def put_own(at, value):
        OWN[:, at : at + step] = value

    def grads(xx, zz):
        at = piece(xx, zz)
        return dot(GT[...], S[0, 0:total, at]), dot(HT[...], S[1, 0:total, at])

    gu_rows, all_rows = 2 * TILE, 3 * TILE
    mid = all_rows // 2
    order = [turn(zl, s, nz) for s in range(1, nz)] + [zl]
    g2_in, g1_in, gz_in = {}, {}, []

    def send_far(i):
        if nx == 1:
            return
        first, second = grads(turn(x, 2, nx), order[i])
        G2[i, 0:gu_rows, :] = first.astype(BF16)
        G2[i, gu_rows:all_rows, :] = second.astype(BF16)
        g2_in[i] = {
            s: net.send(G2.at[i, part * mid : (part + 1) * mid], R2.at[part, i], x=xs[s])
            for s, part in ((1, 0), (-1, 1))
        }

    def send_near(i):
        if nx == 1:
            return
        arrive(g2_in[i], f"g2_{i}")
        copies = {}
        for s, part in ((1, 0), (-1, 1)):
            first, second = grads(xs[s], order[i])
            G = jnp.concatenate([first, second], axis=0)
            lo, hi = part * mid, (part + 1) * mid
            G1[part, i, lo:hi, :] = (G[lo:hi] + R2[part, i].astype(F32)).astype(BF16)
            lo, hi = (1 - part) * mid, (2 - part) * mid
            G1[part, i, lo:hi, :] = G[lo:hi].astype(BF16)
            copies[s] = net.send(G1.at[part, i], R1.at[part, i], x=xs[s])
        g1_in[i] = copies

    def summed_here(i):
        first, second = grads(x, order[i])
        GO[0:gu_rows, :] = first
        GO[gu_rows:all_rows, :] = second
        if nx > 1:
            arrive(g1_in[i], f"g1_{i}")
            GO[...] += R1[0, i].astype(F32) + R1[1, i].astype(F32)

    def to_zl(i):
        if i < nz - 1:
            summed_here(i)
            GS[i] = GO[...].astype(BF16)
            gz_in.append(net.send(GS.at[i], GR.at[i], zl=order[i]))

    quarter = half // 2
    quarters = [slice(q * quarter, (q + 1) * quarter) for q in (0, 1)]
    y_in = {}

    def y_step(t):
        for kind in (0, 1):
            for s, part in ((1, 0), (-1, 1)):
                far = hops + 1 - t - kind
                if far < 1:
                    continue
                q = quarters[part if kind == 0 else 1 - part]
                value = OWN[yrows(turn(y, s * far, ny)), q]
                if t > 1:
                    got(y_in[kind, s], f"r{t}")
                    value = value + YR[part, kind, t - 2].astype(F32)
                YS[part, kind, t - 1] = value.astype(BF16)
                y_in[kind, s] = net.send(
                    YS.at[part, kind, t - 1], YR.at[part, kind, t - 1], y=ys[s]
                )

    send_far(0)
    back_part(other, put_sent)
    c_in = net.send(CX, CR, core=other)
    if nz > 1:
        send_far(1)
    back_part(core, put_own)
    got(c_in, "c")
    OWN[...] += CR[...].astype(F32)
    if hops > 0:
        y_step(1)
    send_near(0)
    if nz > 2:
        send_far(2)
    if hops > 1:
        y_step(2)
    if nz > 1:
        send_near(1)
    if hops > 2:
        y_step(3)
    to_zl(0)
    if hops > 3:
        y_step(4)
    if nz > 2:
        send_near(2)

    mine_y = [OWN[yrows(y), q] for q in quarters]
    for kind in (0, 1):
        for s, part in ((1, 0), (-1, 1)):
            if hops > kind:
                got(y_in[kind, s], "rlast")
                q = part if kind == 0 else 1 - part
                mine_y[q] = mine_y[q] + YR[part, kind, hops - 1 - kind].astype(F32)
    for q in (0, 1):
        spread_rows = dot(pack, mine_y[q].astype(BF16), ((0,), (0,)))
        ZS[:, :, quarters[q]] = spread_rows.reshape(nh, PAD, quarter).astype(BF16)

    if nh > 1:
        pl.semaphore_wait(known, 2)
        z_in = []
        for i, s in enumerate((2, 1, -1)):
            there = turn(zh, s, nh)
            z_in.append(net.send(ZS.at[there], ZR.at[i], zh=there))
    to_zl(1)

    final = ZS[zh].astype(F32)
    if nh > 1:
        for i in (1, 2, 0):
            got(z_in[i], f"rz{i}")
        for i in range(3):
            final = final + ZR[i].astype(F32)
    FR[core] = final.astype(BF16)
    f_in = net.send(FR.at[core], FR.at[core], core=other)

    summed_here(nz - 1)
    for i, copy in enumerate(gz_in):
        got(copy, f"gz{i}")
        GO[...] += GR[i].astype(F32)
    for k in range(3):
        wg_ref[k] = GO[k * TILE : (k + 1) * TILE, :].T

    got(f_in, "f")
    hit_b = HIT[...].astype(BF16)
    for c in (0, 1):
        ig_ref[:, c * half : (c + 1) * half] = dot(hit_b, FR[c], ((0,), (0,))).astype(BF16)

    for copy in net.copies:
        copy.wait_send()


def per_device(sizes, out_grad, layer_input, expert_ids, gate_prob, w_stack, scale_exps):
    nx, nz, ny, nh, _ = sizes
    tokens, d = layer_input.shape
    block = w_stack.shape[1]
    half, rows, wide = d // 2, 6 * nh, 3 * TILE
    total = rows * ny
    hops = max(ny // 2, 1)
    held = total + 8 if total % 16 == 0 else total
    vmem = pl.BlockSpec(memory_space=pltpu.VMEM)
    arrays = (
        out_grad,
        layer_input,
        expert_ids.T,
        gate_prob.T,
        w_stack,
        jnp.transpose(scale_exps, (1, 2, 0)),
    )
    scratch = [pltpu.VMEM(a.shape, a.dtype) for a in arrays] + [
        pltpu.VMEM((d, wide), BF16),
        pltpu.VMEM((2, PAD, d), BF16),
        pltpu.VMEM((PAD, d), BF16),
        pltpu.VMEM((PAD, tokens), F32),
        pltpu.VMEM((nh, PAD, d), BF16),
        pltpu.VMEM((2, held, d), BF16),
        pltpu.VMEM((total, 2 * TILE), BF16),
        pltpu.VMEM((2 * TILE, total), BF16),
        pltpu.VMEM((TILE, total), BF16),
        pltpu.VMEM((total, half), BF16),
        pltpu.VMEM((total, half), BF16),
        pltpu.VMEM((total, half), F32),
        pltpu.VMEM((2, 2, hops, rows, half // 2), BF16),
        pltpu.VMEM((2, 2, hops, rows, half // 2), BF16),
        pltpu.VMEM((nh, PAD, half), BF16),
        pltpu.VMEM((3, PAD, half), BF16),
        pltpu.VMEM((2, PAD, half), BF16),
        pltpu.VMEM((nz, wide, block), BF16),
        pltpu.VMEM((2, nz, wide // 2, block), BF16),
        pltpu.VMEM((2, nz, wide, block), BF16),
        pltpu.VMEM((2, nz, wide, block), BF16),
        pltpu.VMEM((wide, block), F32),
        pltpu.VMEM((nz, wide, block), BF16),
        pltpu.VMEM((nz, wide, block), BF16),
        pltpu.SemaphoreType.DMA((96,)),
        pltpu.SemaphoreType.DMA((96,)),
        pltpu.SemaphoreType.DMA((6,)),
        pltpu.SemaphoreType.REGULAR,
    ]
    return pl.pallas_call(
        functools.partial(kernel, sizes),
        out_shape=(
            jax.ShapeDtypeStruct((tokens, d), BF16),
            jax.ShapeDtypeStruct(w_stack.shape, F32),
        ),
        in_specs=[pl.BlockSpec(memory_space=pltpu.HBM)] * 6,
        out_specs=(vmem, vmem),
        scratch_shapes=scratch,
        compiler_params=pltpu.CompilerParams(
            collective_id=0, has_side_effects=True, vmem_limit_bytes=67043328
        ),
        name="expert_backward",
    )(*arrays)


def build(devices, sizes):
    split = Mesh(devices.reshape(sizes), AXES)
    tokens = P(AXES, None)
    weights = P(None, ("x", "zl"), ("y", "zh", "core"))
    return jax.shard_map(
        functools.partial(per_device, sizes),
        mesh=split,
        in_specs=(tokens, tokens, tokens, tokens, weights, weights),
        out_specs=(tokens, weights),
        check_vma=False,
    )


def solution(mesh):
    return build(mesh.devices, SIZES)
```

```python
import functools

import jax
import jax.numpy as jnp
from jax import lax
from jax.experimental import pallas as pl
from jax.experimental.pallas import tpu as pltpu
from jax.sharding import Mesh
from jax.sharding import PartitionSpec as P

TILE = 128
CAP = 3
PAD = 8
MESH = pl.DeviceIdType.MESH
AXES = ("x", "zl", "y", "zh", "core")
SIZES = (4, 3, 8, 4, 2)
F32 = jnp.float32
BF16 = jnp.bfloat16


def dot(left, right, contract=((1,), (0,))):
    return lax.dot_general(left, right, (contract, ((), ())), preferred_element_type=F32)


class Net:
    def __init__(self, send_sems, recv_sems):
        self.send_sems, self.recv_sems, self.copies = send_sems, recv_sems, []

    def send(self, src, dst, **where):
        i = len(self.copies)
        copy = pltpu.make_async_remote_copy(
            src_ref=src,
            dst_ref=dst,
            send_sem=self.send_sems.at[i],
            recv_sem=self.recv_sems.at[i],
            device_id=where,
            device_id_type=MESH,
        )
        copy.start()
        self.copies.append(copy)
        return copy


def kernel(
    sizes, og_hbm, li_hbm, ids_hbm, prob_hbm, w_hbm, exp_hbm, ig_ref, wg_ref,
    og_ref, li_ref, ids_ref, prob_ref, w_ref, exp_ref,
    W, A, AR, HIT, S, GU, GP, GT, HT, CX, CR, OWN, YS, YR, ZS, ZR, FR,
    G2, R2, G1, R1, GO, GS, GR, DS, DR, DG, D2, E2, D1, E1,
    send_sems, recv_sems, load_sems, known,
):
    nx, nz, ny, nh, _ = sizes
    x, zl, y, zh, core = (lax.axis_index(a) for a in AXES)
    d = li_ref.shape[1]
    half = d // 2
    rows, block = PAD * nh, w_ref.shape[1]
    total = rows * ny
    hops = ny // 2
    net = Net(send_sems, recv_sems)

    def turn(at, by, n):
        return lax.rem(at + by + n, n)

    xs = {s: turn(x, s, nx) for s in (1, -1)}
    ys = {s: turn(y, s, ny) for s in (1, -1)}
    hs = {s: turn(zh, s, nh) for s in (1, -1)}
    other = 1 - core
    both = ((1, 0), (-1, 1))

    barrier = pltpu.get_barrier_semaphore()
    greeted = [dict(core=other)]
    if nx > 1:
        greeted += [dict(x=xs[1]), dict(x=xs[-1])]
    greeted += [dict(zl=turn(zl, s, nz)) for s in range(1, nz)]
    if ny > 1:
        greeted += [dict(y=ys[1]), dict(y=ys[-1])]
    if nh > 1:
        greeted += [dict(zh=hs[1]), dict(zh=hs[-1])]
    for where in greeted:
        pl.semaphore_signal(barrier, inc=1, device_id=where, device_id_type=MESH)

    pairs = [
        (w_hbm, w_ref), (exp_hbm, exp_ref), (ids_hbm, ids_ref), (prob_hbm, prob_ref),
        (li_hbm, li_ref), (og_hbm, og_ref),
    ]
    loads = [pltpu.make_async_copy(src, dst, load_sems.at[i]) for i, (src, dst) in enumerate(pairs)]
    for load in loads:
        load.start()

    def piece(xx, zz):
        return pl.ds(pl.multiple_of((xx * nz + zz) * block, block), block)

    def halfpiece(xx, zz, part):
        size = block // 2
        return pl.ds(pl.multiple_of((xx * nz + zz) * block + part * size, size), size)

    def got(copy, name):
        with jax.named_scope(name):
            copy.wait_recv()

    def arrive(copies, name):
        for s in (1, -1):
            if copies is not None:
                got(copies[s], name)

    for load in loads[2:]:
        load.wait()
    tokens = ids_ref.shape[1]
    r0, r1 = ids_ref[0:1, :] == 0, ids_ref[1:2, :] == 0
    routed = jnp.broadcast_to(jnp.where(r0 | r1, 1.0, 0.0).astype(F32), (PAD, tokens))
    prob = jnp.where(r0, prob_ref[0:1, :], 0.0) + jnp.where(r1, prob_ref[1:2, :], 0.0)
    upto = (
        lax.broadcasted_iota(jnp.int32, (tokens, tokens), 0)
        <= lax.broadcasted_iota(jnp.int32, (tokens, tokens), 1)
    )
    place = dot(routed.astype(BF16), jnp.where(upto, 1.0, 0.0).astype(BF16))
    wanted = (lax.broadcasted_iota(jnp.int32, (PAD, tokens), 0) - CAP * core + 1).astype(F32)
    hit = jnp.where(place == wanted, routed, 0.0)
    HIT[...] = hit
    hit_b = hit.astype(BF16)
    A[0] = dot(hit_b, li_ref[...]).astype(BF16)
    slot_prob = jnp.sum(hit * prob, axis=1, keepdims=True)
    A[1] = (slot_prob * dot(hit_b, og_ref[...])).astype(BF16)

    for load in loads[:2]:
        load.wait()
    for k in range(3):
        for t in range(block // TILE):
            e = exp_ref[t, :, k : k + 1]
            factor = jnp.where(e > 0, 2.0, jnp.where(e < 0, 0.5, 1.0)).astype(F32)
            scaled = (w_ref[k, t * TILE : (t + 1) * TILE, :].astype(F32) * factor).astype(BF16)
            at = pl.multiple_of((x * nz + zl) * block + t * TILE, TILE)
            W[pl.ds(at, TILE), k * TILE : (k + 1) * TILE] = scaled

    with jax.named_scope("greet"):
        pl.semaphore_wait(barrier, len(greeted))
    if nh > 1:
        for s in (1, -1):
            pl.semaphore_signal(known, inc=1, device_id=dict(zh=hs[s]), device_id_type=MESH)

    gu_lanes, all_lanes, down_lanes = slice(0, 2 * TILE), slice(0, 3 * TILE), slice(2 * TILE, 3 * TILE)
    a_in = net.send(A.at[other], AR, core=other)

    def spread(zz, lanes):
        if nx == 1:
            return None
        ref = W.at[piece(x, zz), lanes]
        return {s: net.send(ref, ref, x=xs[s]) for s in (1, -1)}

    def relay(zz, lanes):
        if nx == 1:
            return None
        out = {}
        for s, part in both:
            ref = W.at[halfpiece(xs[-s], zz, part), lanes]
            out[s] = net.send(ref, ref, x=xs[s])
        return out

    def own_to_zl(i):
        ref = W.at[piece(x, zl), all_lanes]
        return net.send(ref, ref, zl=turn(zl, i, nz))

    down_in = []

    def down_to_zl(rows_at):
        for i in range(1, nz):
            ref = W.at[rows_at, down_lanes]
            down_in.append(net.send(ref, ref, zl=turn(zl, i, nz)))

    def sub(yy, hh):
        return pl.ds(pl.multiple_of((yy * nh + hh) * PAD, PAD), PAD)

    def yrows(yy):
        return pl.ds(pl.multiple_of(yy * rows, rows), rows)

    cols = [slice(k * half, (k + 1) * half) for k in (0, 1)]
    every = slice(0, d)
    partner = []

    def to_partner(yy):
        ref = S.at[core, yrows(yy)]
        partner.append(net.send(ref, ref, core=other))

    flows = {}

    def y_start(b, hh):
        if ny > 1:
            ref = S.at[core, sub(y, hh)]
            flows[b] = {s: net.send(ref, ref, y=ys[s]) for s in (1, -1)}

    def y_hop(b, hh, hop):
        if hop > hops:
            return
        for s, part in both:
            got(flows[b][s], f"y{b}_{hop}")
            if hop < hops:
                c = every if hop < hops - 1 else cols[part]
                ref = S.at[core, sub(turn(y, -s * hop, ny), hh), c]
                flows[b][s] = net.send(ref, ref, y=ys[s])
        if b == 3:
            to_partner(turn(y, -hop, ny))
            if hop < hops:
                to_partner(turn(y, hop, ny))

    w_x = {0: spread(zl, all_lanes)}
    w_far, w_z = {}, {}
    zs = [zl] + [turn(zl, -i, nz) for i in range(1, nz)]

    def relay_row(i):
        if i < nz:
            arrive(w_x[i], f"wx{i}")
            w_far[i] = relay(zs[i], all_lanes if i == 0 else gu_lanes)

    def spread_row(i):
        if i < nz:
            got(w_z[i], f"wz{i}")
            w_x[i] = spread(zs[i], gu_lanes)

    got(a_in, "a")
    S[core, sub(y, zh), :] = A[core] + AR[...]
    if nh > 1:
        ref = S.at[core, sub(y, zh)]
        z_in = {s: net.send(ref, ref, zh=hs[s]) for s in (1, -1)}
    if nz > 1:
        w_z[1] = own_to_zl(1)
    b_hh = [zh, hs[-1], hs[1], turn(zh, 2, nh)]
    near = (1, 2) if nh > 1 else ()

    def y_near(hop):
        for b in near:
            y_hop(b, b_hh[b], hop)

    y_start(0, zh)
    y_hop(0, zh, 1)
    relay_row(0)
    if nh > 1:
        arrive(z_in, "zh")
        z_far = []
        for s, part in both:
            ref = S.at[core, sub(y, hs[-s]), cols[part]]
            z_far.append(net.send(ref, ref, zh=hs[s]))
    if nz > 2:
        w_z[2] = own_to_zl(2)
    for b in near:
        y_start(b, b_hh[b])
    if nx > 1:
        for s in (1, -1):
            down_to_zl(piece(xs[s], zl))
    y_hop(0, zh, 2)
    y_near(1)
    y_hop(0, zh, 3)
    spread_row(1)
    if nh > 1:
        for copy in z_far:
            got(copy, "zfar")
        y_start(3, b_hh[3])
        to_partner(y)
    if nx > 1:
        arrive(w_far[0], "wf0")
        down_to_zl(piece(turn(x, 2, nx), zl))
    y_near(2)
    y_hop(0, zh, 4)
    if nh > 1:
        y_hop(3, b_hh[3], 1)
    relay_row(1)
    spread_row(2)
    y_near(3)
    if nh > 1:
        y_hop(3, b_hh[3], 2)
    y_near(4)
    relay_row(2)
    if nh > 1:
        y_hop(3, b_hh[3], 3)
        y_hop(3, b_hh[3], 4)
    else:
        for hop in range(1, hops + 1):
            to_partner(turn(y, -hop, ny))
            if hop < hops:
                to_partner(turn(y, hop, ny))
        to_partner(y)

    for i in range(1, nz):
        arrive(w_far[i], "wfar")
    for copy in down_in:
        got(copy, "down")
    for copy in partner:
        got(copy, "partner")

    def pack(blocks):
        shape = (2 * CAP * blocks, PAD * blocks)
        i, j = (lax.broadcasted_iota(jnp.int32, shape, k) for k in (0, 1))
        return jnp.where(j == (i // (2 * CAP)) * PAD + lax.rem(i, 2 * CAP), 1.0, 0.0).astype(BF16)

    gate_up = dot(S[0, 0:total, :], W[:, gu_lanes])
    back = dot(S[1, 0:total, :], W[:, down_lanes])
    gate, up = gate_up[:, 0:TILE], gate_up[:, TILE : 2 * TILE]
    sig = jax.nn.sigmoid(gate)
    act = gate * sig
    gate_grad = back * up * sig * (1.0 + gate * (1.0 - sig))
    up_grad = back * act
    GU[:, 0:TILE] = gate_grad.astype(BF16)
    GU[:, TILE : 2 * TILE] = up_grad.astype(BF16)
    GP[...] = dot(pack(ny * nh), GU[...]).astype(BF16)
    GT[0:TILE, :] = gate_grad.T.astype(BF16)
    GT[TILE : 2 * TILE, :] = up_grad.T.astype(BF16)
    HT[...] = (act * up).T.astype(BF16)

    step = block if half % block == 0 else TILE

    def back_part(which, put):
        for j in range(half // step):
            at = pl.multiple_of(which * half + j * step, step)
            put(j * step, dot(GP[...], W[pl.ds(at, step), gu_lanes], ((1,), (1,))))

    def put_sent(at, value):
        CX[:, at : at + step] = value.astype(BF16)

    def put_own(at, value):
        OWN[:, at : at + step] = value

    def gu_grad(xx, zz):
        return dot(GT[...], S[0, 0:total, piece(xx, zz)])

    def down_grad(xx, zz):
        return dot(HT[...], S[1, 0:total, piece(xx, zz)])

    order = [turn(zl, i, nz) for i in range(1, nz)] + [zl]
    g2_in, g1_in, gz_in, dz_in = {}, {}, [], []

    def send_far(i):
        if nx == 1 or i >= nz:
            return
        G2[i] = gu_grad(turn(x, 2, nx), order[i]).astype(BF16)
        g2_in[i] = {
            s: net.send(G2.at[i, part * TILE : (part + 1) * TILE], R2.at[part, i], x=xs[s])
            for s, part in both
        }

    def send_near(i):
        if nx == 1 or i >= nz:
            return
        arrive(g2_in[i], f"g2_{i}")
        copies = {}
        for s, part in both:
            G = gu_grad(xs[s], order[i])
            lo, hi = part * TILE, (part + 1) * TILE
            G1[part, i, lo:hi, :] = (G[lo:hi] + R2[part, i].astype(F32)).astype(BF16)
            lo, hi = (1 - part) * TILE, (2 - part) * TILE
            G1[part, i, lo:hi, :] = G[lo:hi].astype(BF16)
            copies[s] = net.send(G1.at[part, i], R1.at[part, i], x=xs[s])
        g1_in[i] = copies

    def summed_here(i):
        G = gu_grad(x, order[i])
        if nx > 1:
            arrive(g1_in[i], f"g1_{i}")
            G = G + R1[0, i].astype(F32) + R1[1, i].astype(F32)
        return G

    def to_zl(i):
        if i < nz - 1:
            GS[i] = summed_here(i).astype(BF16)
            gz_in.append(net.send(GS.at[i], GR.at[i], zl=order[i]))

    def down_zl(i):
        if i < nz - 1:
            for xx in range(nx):
                DS[i, xx] = down_grad(xx, order[i]).astype(BF16)
            dz_in.append(net.send(DS.at[i], DR.at[i], zl=order[i]))

    few = 2 * CAP * nh

    def fewrows(yy):
        return pl.ds(pl.multiple_of(yy * few, few), few)

    quarter = half // 2
    quarters = [slice(q * quarter, (q + 1) * quarter) for q in (0, 1)]
    y_in = {}

    def y_step(t):
        for kind in (0, 1):
            for s, part in both:
                far = hops + 1 - t - kind
                if far < 1:
                    continue
                q = quarters[part if kind == 0 else 1 - part]
                value = OWN[fewrows(turn(y, s * far, ny)), q]
                if t > 1:
                    got(y_in[kind, s], f"r{t}")
                    value = value + YR[part, kind, t - 2].astype(F32)
                YS[part, kind, t - 1] = value.astype(BF16)
                y_in[kind, s] = net.send(
                    YS.at[part, kind, t - 1], YR.at[part, kind, t - 1], y=ys[s]
                )

    back_part(other, put_sent)
    c_in = net.send(CX, CR, core=other)
    send_far(0)
    down_zl(0)
    send_far(1)
    back_part(core, put_own)
    got(c_in, "c")
    OWN[...] += CR[...].astype(F32)
    y_step(1)
    down_zl(1)
    send_far(2)
    send_near(0)
    for xx in range(nx):
        DG[xx] = down_grad(xx, zl)
    y_step(2)
    send_near(1)
    y_step(3)
    to_zl(0)
    y_step(4)
    send_near(2)

    mine_y = [OWN[fewrows(y), q] for q in quarters]
    for kind in (0, 1):
        for s, part in both:
            if hops > kind:
                got(y_in[kind, s], "rlast")
                q = part if kind == 0 else 1 - part
                mine_y[q] = mine_y[q] + YR[part, kind, hops - 1 - kind].astype(F32)
    for q in (0, 1):
        spread_rows = dot(pack(nh), mine_y[q].astype(BF16), ((0,), (0,)))
        ZS[:, :, quarters[q]] = spread_rows.reshape(nh, PAD, quarter).astype(BF16)

    if nh > 1:
        pl.semaphore_wait(known, 2)
        z_in = []
        for i, s in enumerate((2, 1, -1)):
            there = turn(zh, s, nh)
            z_in.append(net.send(ZS.at[there], ZR.at[i], zh=there))
    to_zl(1)

    for i, copy in enumerate(dz_in):
        got(copy, f"dz{i}")
        DG[...] += DR[i].astype(F32)
    mid = TILE // 2
    if nx > 1:
        D2[...] = DG[turn(x, 2, nx)].astype(BF16)
        d_in = {
            s: net.send(D2.at[part * mid : (part + 1) * mid], E2.at[part], x=xs[s])
            for s, part in both
        }

    if nx > 1:
        arrive(d_in, "d2")
        for s, part in both:
            lo, hi = part * mid, (part + 1) * mid
            D1[part, lo:hi, :] = (DG[xs[s], lo:hi, :] + E2[part].astype(F32)).astype(BF16)
            lo, hi = (1 - part) * mid, (2 - part) * mid
            D1[part, lo:hi, :] = DG[xs[s], lo:hi, :].astype(BF16)
            d_in[s] = net.send(D1.at[part], E1.at[part], x=xs[s])

    final = ZS[zh].astype(F32)
    if nh > 1:
        for i in (1, 2, 0):
            got(z_in[i], f"rz{i}")
        for i in range(3):
            final = final + ZR[i].astype(F32)
    FR[core] = final.astype(BF16)
    f_in = net.send(FR.at[core], FR.at[core], core=other)

    GO[...] = summed_here(nz - 1)
    for i, copy in enumerate(gz_in):
        got(copy, f"gz{i}")
        GO[...] += GR[i].astype(F32)
    for k in range(2):
        wg_ref[k] = GO[k * TILE : (k + 1) * TILE, :].T

    total_down = DG[x]
    if nx > 1:
        arrive(d_in, "d1")
        total_down = total_down + E1[0].astype(F32) + E1[1].astype(F32)
    wg_ref[2] = total_down.T

    got(f_in, "f")
    hit_b = HIT[...].astype(BF16)
    for c in (0, 1):
        ig_ref[:, cols[c]] = dot(hit_b, FR[c], ((0,), (0,))).astype(BF16)

    for copy in net.copies:
        copy.wait_send()


def per_device(sizes, out_grad, layer_input, expert_ids, gate_prob, w_stack, scale_exps):
    nx, nz, ny, nh, _ = sizes
    tokens, d = layer_input.shape
    block = w_stack.shape[1]
    half, rows, wide = d // 2, PAD * nh, 2 * TILE
    total = rows * ny
    hops, few = max(ny // 2, 1), 2 * CAP * nh
    arrays = (
        out_grad,
        layer_input,
        expert_ids.T,
        gate_prob.T,
        w_stack,
        jnp.transpose(scale_exps, (1, 2, 0)),
    )
    outs = (jax.ShapeDtypeStruct((tokens, d), BF16), jax.ShapeDtypeStruct(w_stack.shape, F32))
    scratch = [pltpu.VMEM(a.shape, a.dtype) for a in arrays] + [
        pltpu.VMEM((d, 3 * TILE), BF16),
        pltpu.VMEM((2, PAD, d), BF16),
        pltpu.VMEM((PAD, d), BF16),
        pltpu.VMEM((PAD, tokens), F32),
        pltpu.VMEM((2, total + PAD, d), BF16),
        pltpu.VMEM((total, wide), BF16),
        pltpu.VMEM((few * ny, wide), BF16),
        pltpu.VMEM((wide, total), BF16),
        pltpu.VMEM((TILE, total), BF16),
        pltpu.VMEM((few * ny, half), BF16),
        pltpu.VMEM((few * ny, half), BF16),
        pltpu.VMEM((few * ny, half), F32),
        pltpu.VMEM((2, 2, hops, few, half // 2), BF16),
        pltpu.VMEM((2, 2, hops, few, half // 2), BF16),
        pltpu.VMEM((nh, PAD, half), BF16),
        pltpu.VMEM((3, PAD, half), BF16),
        pltpu.VMEM((2, PAD, half), BF16),
        pltpu.VMEM((nz, wide, block), BF16),
        pltpu.VMEM((2, nz, TILE, block), BF16),
        pltpu.VMEM((2, nz, wide, block), BF16),
        pltpu.VMEM((2, nz, wide, block), BF16),
        pltpu.VMEM((wide, block), F32),
        pltpu.VMEM((nz, wide, block), BF16),
        pltpu.VMEM((nz, wide, block), BF16),
        pltpu.VMEM((nz, nx, TILE, block), BF16),
        pltpu.VMEM((nz, nx, TILE, block), BF16),
        pltpu.VMEM((nx, TILE, block), F32),
        pltpu.VMEM((TILE, block), BF16),
        pltpu.VMEM((2, TILE // 2, block), BF16),
        pltpu.VMEM((2, TILE, block), BF16),
        pltpu.VMEM((2, TILE, block), BF16),
        pltpu.SemaphoreType.DMA((128,)),
        pltpu.SemaphoreType.DMA((128,)),
        pltpu.SemaphoreType.DMA((6,)),
        pltpu.SemaphoreType.REGULAR,
    ]
    hbm = pl.BlockSpec(memory_space=pltpu.HBM)
    return pl.pallas_call(
        functools.partial(kernel, sizes),
        out_shape=outs,
        in_specs=[hbm] * 6,
        out_specs=(pl.BlockSpec(memory_space=pltpu.VMEM),) * 2,
        scratch_shapes=scratch,
        compiler_params=pltpu.CompilerParams(
            collective_id=0, has_side_effects=True, vmem_limit_bytes=67043328
        ),
        name="expert_backward",
    )(*arrays)


def build(devices, sizes):
    split = Mesh(devices.reshape(sizes), AXES)
    tokens = P(AXES, None)
    weights = P(None, ("x", "zl"), ("y", "zh", "core"))
    return jax.shard_map(
        functools.partial(per_device, sizes),
        mesh=split,
        in_specs=(tokens, tokens, tokens, tokens, weights, weights),
        out_specs=(tokens, weights),
        check_vma=False,
    )


def solution(mesh):
    return build(mesh.devices, SIZES)
```
